32 devices in a mesh: row: 8 (over z, x), col: 4 (over y, core).
Axes of the slice: x: 2, y: 2, z: 4, core: 2. Of those that a mesh axis runs over, the one named last changes fastest.
Arguments:
- panel_block: float32 [20480, 512], P('row', 'col'), may hold values from -12 to 12
- trailing: float32 [20480, 20480], P('row', 'col'), may hold values from -6 to 6
Outputs:
- updated: float32 [20480, 20480], P('row', 'col')
The draws below stay inside these ranges and needn't reach their ends.
All inputs are finite; a program needn't handle non-finite values.
Results may differ from the reference program's by a relative error of at most 0.0003.
Values sent between devices are 32-bit elements; how exact they have to be, the bound alone decides.
No kernel may reach another device: no remote copies, remote signals or barrier semaphores. Data moves between devices by JAX's collectives and lax.ppermute only.
A program may use at most 192 MiB of HBM per device.

```python
import math
import jax
import jax.numpy as jnp
from jax import lax

N = 20480
K = 512
N_ROW = 8
N_COL = 4


def draw_panel_block(key, part):
    subkeys = jax.random.split(jax.random.fold_in(key, 11), 3)
    position = jnp.arange(N, dtype=jnp.float32) / N
    rising = 3.0 ** (position - 0.5)
    entries = jax.random.normal(subkeys[0], (N, K), jnp.float32)
    spread = 0.5
    row_scale = 10.0 ** jax.random.uniform(subkeys[1], (N, 1), jnp.float32, -spread, spread)
    col_scale = 10.0 ** jax.random.uniform(subkeys[2], (1, K), jnp.float32, -spread, spread)
    return entries * rising[:, None] * row_scale * col_scale / math.sqrt(K)


def steps_of(stream_key, dims, shards, low, top_value):
    gain, own = 1.0, jax.random.fold_in(stream_key, 6)
    for dim, blocks in shards:
        draws = jnp.exp(jax.random.uniform(jax.random.fold_in(own, dim), (blocks,), jnp.float32, low / len(shards), top_value / len(shards)))
        gain = gain * jnp.repeat(draws, dims[dim] // blocks).reshape([-1 if axis == dim else 1 for axis in range(len(dims))])
    return gain


def centred(own_key, shape, deviation, most, cuts=(), kind=jnp.bfloat16):
    values = deviation * jax.random.normal(own_key, shape, jnp.float32)
    if cuts:
        values = values * steps_of(own_key, shape, cuts, -0.22, 0.18)
    return jnp.clip(values, -most, most).astype(kind)


def setup_inputs(seed: int = 0) -> dict:
    seeds = jax.random.split(jax.random.key(seed), 3)
    panel_block = draw_panel_block(jax.random.fold_in(seeds[2], 71), 0)
    trailing = centred(seeds[1], (N, N), 1.0, 6.0, ((0, 8), (1, 4)), jnp.float32)
    return {"panel_block": panel_block, "trailing": trailing}


def reference(panel_block, trailing):
    local_rows = N // N_ROW
    local_cols = N // N_COL
    squares = jnp.sum(panel_block * panel_block)
    factor = 0.8 * jnp.sqrt(jnp.float32(N)) / jnp.sqrt(squares + 1e-06)
    matrix = panel_block.reshape(N_ROW, local_rows, K).transpose(1, 0, 2).reshape(N, K)
    column_rows = matrix.reshape(local_cols, N_COL, K).transpose(1, 0, 2).reshape(N, K)
    position = jnp.arange(N, dtype=jnp.int32)
    col_index = position % local_cols * N_COL + position // local_cols

    def one_block(pieces):
        row_block, slab_rows, source = pieces
        update = lax.dot_general(row_block, column_rows, (((1,), (1,)), ((), ())), precision=lax.Precision.HIGHEST, preferred_element_type=jnp.float32)
        row_index = jnp.arange(local_rows, dtype=jnp.int32) * N_ROW + source
        lower_part = row_index[:, None] >= col_index[None, :]
        return slab_rows - factor * jnp.where(lower_part, update, jnp.zeros_like(update))
    blocks = lax.map(one_block, (panel_block.reshape(N_ROW, local_rows, K), trailing.reshape(N_ROW, local_rows, N), jnp.arange(N_ROW, dtype=jnp.int32)))
    return blocks.reshape(N, N)
```

```python
import jax
import jax.numpy as jnp
from jax import lax
from jax.experimental import pallas as pl
from jax.experimental.pallas import tpu as pltpu
from jax.sharding import PartitionSpec as P

SLABS = 4
TILES_PER_SLAB = 2


def split(x):
    hi = x.astype(jnp.bfloat16)
    lo = (x - hi.astype(jnp.float32)).astype(jnp.bfloat16)
    return hi, lo


def copy_upper(trailing, tile_rows, slab_cols):
    tiles = [(t, q) for q in range(1, SLABS) for t in range(TILES_PER_SLAB * q)]
    rows = jnp.array([t for t, _ in tiles], jnp.int32)
    cols = jnp.array([q for _, q in tiles], jnp.int32)

    def body(rows_ref, cols_ref, x_ref, o_ref):
        o_ref[...] = x_ref[...]

    spec = pl.BlockSpec((tile_rows, slab_cols), lambda n, rows, cols: (rows[n], cols[n]))
    return pl.pallas_call(
        body,
        grid_spec=pltpu.PrefetchScalarGridSpec(
            num_scalar_prefetch=2, grid=(len(tiles),), in_specs=[spec], out_specs=spec
        ),
        out_shape=jax.ShapeDtypeStruct(trailing.shape, trailing.dtype),
        name="copy_upper",
    )(rows, cols, trailing)


def update_slab(slab, where_am_i, factor, mine, gathered, trailing, out, rows_count, cols_count, copies):
    local_rows, local_cols = trailing.shape
    width = mine[0].shape[1]
    depth = width * cols_count
    slab_cols = local_cols // SLABS
    chunk = slab_cols // copies
    row_tiles = SLABS * TILES_PER_SLAB
    tile_rows = local_rows // row_tiles
    first = slab * TILES_PER_SLAB
    strided = width % 128 == 0
    if not strided:
        mixed = gathered.reshape(copies, cols_count, chunk, width)
        gathered = jnp.transpose(mixed, (1, 2, 0, 3)).reshape(cols_count, slab_cols, width)

    def body(place_ref, factor_ref, *refs):
        mine_refs = refs[:cols_count]
        g_ref, c_ref, _, o_ref, mixed_ref, b_ref, a_ref = refs[cols_count:]
        step = pl.program_id(0)
        row_owner = place_ref[0]
        col_owner = place_ref[1]

        @pl.when(step == 0)
        def _():
            for m in range(cols_count):
                source = col_owner ^ m
                if strided:
                    for s in range(copies):
                        mixed_ref[pl.ds(s, chunk, stride=copies), :] = g_ref[s * cols_count + source]
                    hi, lo = split(mixed_ref[...])
                else:
                    hi, lo = split(g_ref[source])
                b_ref[:, m * width:(m + 1) * width] = hi
                b_ref[:, depth + m * width:depth + (m + 1) * width] = lo
                b_ref[:, 2 * depth + m * width:2 * depth + (m + 1) * width] = hi

        for m in range(cols_count):
            hi, lo = split(mine_refs[m][...])
            a_ref[:, m * width:(m + 1) * width] = hi
            a_ref[:, depth + m * width:depth + (m + 1) * width] = hi
            a_ref[:, 2 * depth + m * width:2 * depth + (m + 1) * width] = lo
        product = lax.dot_general(
            a_ref[...], b_ref[...], (((1,), (1,)), ((), ())), preferred_element_type=jnp.float32
        )
        row = lax.broadcasted_iota(jnp.int32, (tile_rows, 1), 0) + (first + step) * tile_rows
        col = lax.broadcasted_iota(jnp.int32, (1, slab_cols), 1) + slab * slab_cols
        lower = row * rows_count + row_owner >= col * cols_count + col_owner
        o_ref[...] = c_ref[...] - jnp.where(lower, factor_ref[0] * product, 0.0)

    mine_spec = pl.BlockSpec((tile_rows, width), lambda n: (first + n, 0))
    tile_spec = pl.BlockSpec((tile_rows, slab_cols), lambda n: (first + n, slab))
    return pl.pallas_call(
        body,
        grid=(row_tiles - first,),
        in_specs=[
            pl.BlockSpec(memory_space=pltpu.SMEM),
            pl.BlockSpec(memory_space=pltpu.SMEM),
            *[mine_spec] * cols_count,
            pl.BlockSpec(gathered.shape, lambda n: (0, 0, 0)),
            tile_spec,
            pl.BlockSpec(memory_space=pl.ANY),
        ],
        out_specs=tile_spec,
        out_shape=jax.ShapeDtypeStruct(trailing.shape, trailing.dtype),
        scratch_shapes=[
            pltpu.VMEM((slab_cols, width), jnp.float32),
            pltpu.VMEM((slab_cols, 3 * depth), jnp.bfloat16),
            pltpu.VMEM((tile_rows, 3 * depth), jnp.bfloat16),
        ],
        input_output_aliases={cols_count + 4: 0},
        name=f"update_slab_{slab}",
    )(where_am_i, factor, *mine, gathered, trailing, out)


def on_device(panel_block, trailing):
    local_rows, width = panel_block.shape
    local_cols = trailing.shape[1]
    rows_count = lax.axis_size("row")
    cols_count = lax.axis_size("col")
    copies = rows_count // cols_count
    order = local_rows * rows_count
    row_owner = lax.axis_index("row")
    col_owner = lax.axis_index("col")
    chunk = local_rows // SLABS

    moves = []
    for r in range(rows_count):
        for c in range(cols_count):
            to = ((r // cols_count) * cols_count + c) * cols_count + r % cols_count
            moves.append((r * cols_count + c, to))
    moved = [
        lax.ppermute(panel_block[q * chunk:(q + 1) * chunk], ("row", "col"), moves)
        for q in range(SLABS)
    ]
    mine = {0: panel_block}
    bit = cols_count // 2
    while bit:
        pairs = [(c, c ^ bit) for c in range(cols_count)]
        for m in list(mine):
            mine[m ^ bit] = lax.ppermute(mine[m], "col", pairs)
        bit //= 2
    mine = [mine[m] for m in range(cols_count)]

    squares = lax.psum(jnp.sum(panel_block * panel_block), ("row", "col"))
    factor = 0.8 * jnp.sqrt(jnp.float32(order)) / jnp.sqrt(squares + 1e-06)
    where_am_i = jnp.stack([row_owner, col_owner]).astype(jnp.int32)

    out = copy_upper(trailing, local_rows // (SLABS * TILES_PER_SLAB), local_cols // SLABS)
    for q in range(SLABS):
        gathered = lax.all_gather(moved[q], "row", axis=0, tiled=False)
        out = update_slab(
            q, where_am_i, factor.reshape(1), mine, gathered, trailing, out, rows_count, cols_count, copies
        )
    return out


def solution(mesh):
    in_specs = (P("row", "col"), P("row", "col"))
    out_specs = P("row", "col")
    return jax.shard_map(
        on_device, mesh=mesh, in_specs=in_specs, out_specs=out_specs, check_vma=False
    )
```
